128 devices in a mesh: row: 8 (over z, core), col: 16 (over y, x).
Axes of the slice: x: 4, y: 4, z: 4, core: 2. Of those that a mesh axis runs over, the one named last changes fastest.
Arguments:
- src_field: bfloat16 [64, 4194304], P(None, ('row', 'col')), may hold values from 0.5 to 2
- src_area: float32 [4194304], P(('row', 'col')), may hold values from 0.3 to 3
- tgt_area: float32 [1048576], P(('row', 'col')), may hold values from 0.3 to 3
- weights: bfloat16 [49152, 128, 128], P(('row', 'col')), may hold values from 0 to 0.0025939941
- send_index: int32 [128, 128, 2], P(('row', 'col')), may hold values from -1 to 255, as said below
- pair_slot: int32 [49152], P(('row', 'col')), may hold values from 0 to 255, as said below
- pair_target: int32 [49152], P(('row', 'col')), may hold values from 0 to 63, as said below
Outputs:
- target_field: float32 [64, 1048576], P(None, ('row', 'col'))
The draws below stay inside these ranges and needn't reach their ends.
Inputs may be any that keep to these rules, and one draw needn't show every extreme that they name: `send_index`: in each [s, r] the live entries (not -1) come first and there are 1 to 2 of them; every sender sends to every receiver; for each receiver some sender fills all 2 slots. `pair_slot`: each pair of device r names a live slot of what device r receives; every live slot is named by some pair of device r. `pair_target`: every local target block of a device is named by some pair of that device.
All inputs are finite; a program needn't handle non-finite values.
Results may differ from the reference program's by a relative error of at most 0.0003.
Values may be sent and summed in bfloat16 or wider, within the bound.
A program may use at most 128 MiB of HBM per device.

```python
import math
import jax
import jax.numpy as jnp
from jax import lax

VARS = 8
LEV = 8
BLK = 128
CAP = 2
SB_DEV = 256
TB_DEV = 64
PAIRS_DEV = 384
NEAR = 128
NSB = 32768
NTB = 8192
PAIRS = 49152
N_ROW = 8
N_COL = 16


def routing(key):
    peer_count = N_ROW * N_COL
    base = jax.random.fold_in(key, 7)
    offsets = jnp.arange(NEAR, dtype=jnp.int32)
    receivers = jnp.arange(peer_count, dtype=jnp.int32)
    senders_of = (receivers[:, None] + offsets[None, :]) % peer_count
    near_counts = jax.random.randint(jax.random.fold_in(base, 1), (peer_count, NEAR), 1, CAP + 1)
    full_near = jax.random.randint(jax.random.fold_in(base, 2), (peer_count,), 0, NEAR)
    near_counts = jnp.where(jnp.arange(NEAR)[None, :] == full_near[:, None], CAP, near_counts)
    receiver_grid = jnp.broadcast_to(receivers[:, None], (peer_count, NEAR))
    counts = jnp.zeros((peer_count, peer_count), jnp.int32).at[senders_of, receiver_grid].set(near_counts)
    local_pick = jax.random.randint(jax.random.fold_in(base, 3), (peer_count, peer_count, CAP), 0, SB_DEV)
    alive_mask = jnp.arange(CAP)[None, None, :] < counts[:, :, None]
    send_index = jnp.where(alive_mask, local_pick, -1).astype(jnp.int32)
    position = jnp.arange(PAIRS_DEV, dtype=jnp.int32)
    near_pos = jnp.minimum(position // CAP, NEAR - 1)
    slot_pos = position % CAP
    first_sender = senders_of[:, near_pos]
    first_count = near_counts[:, near_pos]
    first_pick = jnp.where(slot_pos[None, :] < first_count, first_sender * CAP + slot_pos[None, :], first_sender * CAP)
    extra_near = jax.random.randint(jax.random.fold_in(base, 4), (peer_count, PAIRS_DEV), 0, NEAR)
    extra_raw = jax.random.randint(jax.random.fold_in(base, 6), (peer_count, PAIRS_DEV), 0, CAP)
    extra_sender = jnp.take_along_axis(senders_of, extra_near, axis=1)
    extra_count = jnp.take_along_axis(near_counts, extra_near, axis=1)
    extra_pick = extra_sender * CAP + extra_raw % extra_count
    slots_all = jnp.where((position < NEAR * CAP)[None, :], first_pick, extra_pick)
    targets_all = jnp.broadcast_to((position % TB_DEV)[None, :], (peer_count, PAIRS_DEV))
    shuffle = jax.vmap(lambda sub: jax.random.permutation(sub, PAIRS_DEV))(jax.random.split(jax.random.fold_in(base, 5), peer_count))
    pair_slot = jnp.take_along_axis(slots_all, shuffle, axis=1).reshape(-1).astype(jnp.int32)
    pair_target = jnp.take_along_axis(targets_all, shuffle, axis=1).reshape(-1).astype(jnp.int32)
    return (send_index, pair_slot, pair_target)


def draw_send_index(key, part):
    return routing(key)[0]


def draw_pair_slot(key, part):
    return routing(key)[1]


def draw_pair_target(key, part):
    return routing(key)[2]


def shard_levels(stream_key, dims, cuts, smallest, largest):
    def one(dim, blocks):
        heights = jax.random.uniform(jax.random.fold_in(jax.random.fold_in(stream_key, 6), dim), (blocks,), jnp.float32, smallest / len(cuts), largest / len(cuts))
        return jnp.repeat(jnp.exp(heights), dims[dim] // blocks).reshape((-1,) + (1,) * (len(dims) - dim - 1))

    gain = one(*cuts[0])
    for cut in cuts[1:]:
        gain = gain * one(*cut)
    return gain


def setup_inputs(seed: int = 0) -> dict:
    splits = jax.random.split(jax.random.key(seed), 8)
    src_field = jnp.clip(0.5 + 1.5 * jax.random.uniform(splits[0], (VARS * LEV, NSB * BLK), jnp.float32) ** shard_levels(splits[0], (VARS * LEV, NSB * BLK), ((1, 128),), -0.2, 0.2), 0.5, 2.0).astype(jnp.bfloat16)
    src_area = jnp.clip(jnp.exp(math.log(3.0) - 2.3025851 * jax.random.uniform(splits[1], (NSB * BLK,), jnp.float32) ** shard_levels(splits[1], (NSB * BLK,), ((0, 128),), -0.2, 0.2)), 0.3, 3.0)
    tgt_area = jnp.clip(jnp.exp(math.log(3.0) - 2.3025851 * jax.random.uniform(splits[2], (NTB * BLK,), jnp.float32) ** shard_levels(splits[2], (NTB * BLK,), ((0, 128),), -0.2, 0.2)), 0.3, 3.0)
    weights = jnp.clip(0.0025939941 * jax.random.uniform(splits[3], (PAIRS, BLK, BLK), jnp.float32) ** shard_levels(splits[3], (PAIRS, BLK, BLK), ((0, 128),), -0.2, 0.2), 0.0, 0.0025939941).astype(jnp.bfloat16)
    send_index = draw_send_index(jax.random.fold_in(splits[7], 71), 0)
    pair_slot = draw_pair_slot(jax.random.fold_in(splits[7], 71), 0)
    pair_target = draw_pair_target(jax.random.fold_in(splits[7], 71), 0)
    return {"src_field": src_field, "src_area": src_area, "tgt_area": tgt_area, "weights": weights, "send_index": send_index, "pair_slot": pair_slot, "pair_target": pair_target}


def reference(src_field, src_area, tgt_area, weights, send_index, pair_slot, pair_target):
    peer_count = N_ROW * N_COL
    columns = VARS * LEV
    blocks = src_field.reshape(columns, peer_count * SB_DEV, BLK)

    def per_receiver(receiver):
        slot_ids = lax.dynamic_slice_in_dim(pair_slot, receiver * PAIRS_DEV, PAIRS_DEV)
        targets = lax.dynamic_slice_in_dim(pair_target, receiver * PAIRS_DEV, PAIRS_DEV)
        tiles = lax.dynamic_slice_in_dim(weights, receiver * PAIRS_DEV, PAIRS_DEV, 0)
        sender = slot_ids // CAP
        slot_pos = slot_ids % CAP
        local_ids = send_index[sender, receiver, slot_pos]
        global_ids = (sender * SB_DEV + local_ids).astype(jnp.int32)
        picked = jnp.take(blocks, global_ids, axis=1)
        products = jnp.einsum('cps,pst->pct', picked.astype(jnp.float32), tiles.astype(jnp.float32), precision=lax.Precision.HIGHEST)
        return jax.ops.segment_sum(products, targets, num_segments=TB_DEV)

    regridded = lax.map(per_receiver, jnp.arange(peer_count, dtype=jnp.int32))
    regridded = jnp.transpose(regridded, (2, 0, 1, 3)).reshape(columns, peer_count * TB_DEV * BLK)
    source_mass = jnp.sum(src_field.astype(jnp.float32) * src_area[None, :], axis=1)
    target_mass = jnp.sum(regridded * tgt_area[None, :], axis=1)
    return regridded * (source_mass / target_mass)[:, None]
```

```python
import itertools
import random

import jax
import jax.numpy as jnp
from jax import lax
from jax.experimental import pallas as pl
from jax.experimental.pallas import tpu as pltpu
from jax.sharding import PartitionSpec as P

AXES = ("row", "col")
MESH = pl.DeviceIdType.MESH
PEERS = 128
CAP = 2
BLK = 128
VREG = 64
SB = 256
TB = 64
PAIRS = 384
CHUNKS = 8


def offsets_in_order():
    every = [o for o in itertools.product(range(4), range(4), range(4), range(2)) if any(o)]

    def canon(o):
        forms = [tuple((s * v) % 4 for v in o[p:3] + o[:p]) for p in range(3) for s in (1, -1)]
        return min(forms) + o[3:]

    sets = {}
    for o in every:
        sets.setdefault(canon(o), []).append(o)
    rng = random.Random(5)
    groups = list(sets.values())
    rng.shuffle(groups)
    for g in groups:
        rng.shuffle(g)
    flat = [o for g in groups for o in g]
    return sorted(flat, key=lambda o: sum(v != 0 for v in o))


ORDER = offsets_in_order()
NEAR = [o for o in ORDER if sum(v != 0 for v in o) == 1]
PLANE = [o for o in ORDER if o[2] == 0 and o[3] == 0]


def exchange_kernel(send_ref, src_hbm, inb, src, outb, load_sem, self_sem, ssem, rsem, round_sem):
    row, col = lax.axis_index("row"), lax.axis_index("col")
    me = row * 16 + col
    z, k, y, x = row // 2, lax.rem(row, 2), col // 4, lax.rem(col, 4)

    def peer(o):
        dx, dy, dz, dk = o
        r = lax.rem(z + dz, 4) * 2 + lax.rem(k + dk, 2)
        c = lax.rem(y + dy, 4) * 4 + lax.rem(x + dx, 4)
        return r, c

    def load(b):
        return pltpu.make_async_copy(src_hbm.at[:, pl.ds(pl.multiple_of(b * BLK, BLK), BLK)], src.at[b], load_sem)

    barrier = pltpu.get_barrier_semaphore()
    for o in NEAR:
        pl.semaphore_signal(barrier, inc=1, device_id=peer(o), device_id_type=MESH)

    @pl.loop(0, SB, unroll=8)
    def _(b):
        load(b).start()

    @pl.loop(0, SB, unroll=8)
    def _(b):
        load(b).wait()

    def stage(i, dest):
        for c in range(CAP):
            block = jnp.maximum(send_ref[c, dest], 0)
            outb[i, c] = src[block]

    copies = []

    def send(lo, hi):
        for i in range(lo, hi):
            r, c = peer(ORDER[i])
            cp = pltpu.make_async_remote_copy(
                src_ref=outb.at[i], dst_ref=inb.at[me], send_sem=ssem.at[i], recv_sem=rsem.at[i],
                device_id=(r, c), device_id_type=MESH)
            cp.start()
            copies.append(cp)

    def stage_all(lo, hi):
        for i in range(lo, hi):
            r, c = peer(ORDER[i])
            stage(i, r * 16 + c)

    stage_all(0, 10)
    pl.semaphore_wait(barrier, len(NEAR))
    for o in NEAR:
        pl.semaphore_signal(round_sem.at[0], inc=1, device_id=peer(o), device_id_type=MESH)
    send(0, 10)
    stage_all(10, 46)
    pl.semaphore_wait(round_sem.at[0], len(NEAR))
    for o in PLANE:
        pl.semaphore_signal(round_sem.at[1], inc=1, device_id=peer(o), device_id_type=MESH)
    send(10, 46)
    stage_all(46, 127)
    stage(127, me)
    own = pltpu.make_async_copy(outb.at[127], inb.at[me], self_sem)
    own.start()
    pl.semaphore_wait(round_sem.at[1], len(PLANE))
    send(46, 127)
    own.wait()
    for cp in copies:
        cp.wait_recv()
    for cp in copies:
        cp.wait_send()


def exchange(send_rows, src_field):
    return pl.pallas_call(
        exchange_kernel,
        out_shape=jax.ShapeDtypeStruct((PEERS, CAP, VREG, BLK), jnp.bfloat16),
        in_specs=[pl.BlockSpec(memory_space=pltpu.SMEM), pl.BlockSpec(memory_space=pl.ANY)],
        out_specs=pl.BlockSpec(memory_space=pl.ANY),
        scratch_shapes=[
            pltpu.VMEM((SB, VREG, BLK), jnp.bfloat16),
            pltpu.VMEM((PEERS, CAP, VREG, BLK), jnp.bfloat16),
            pltpu.SemaphoreType.DMA,
            pltpu.SemaphoreType.DMA,
            pltpu.SemaphoreType.DMA((PEERS,)),
            pltpu.SemaphoreType.DMA((PEERS,)),
            pltpu.SemaphoreType.REGULAR((2,)),
        ],
        compiler_params=pltpu.CompilerParams(
            collective_id=0, has_side_effects=True, vmem_limit_bytes=56 * 2**20),
        name="exchange",
    )(send_rows, src_field)


def regrid_kernel(slot_ref, target_ref, inb, weights, area_ref, out_ref, mass_ref, x, w, acc, xsem, wsem):
    load = pltpu.make_async_copy(inb, x, xsem)
    load.start()
    per = PAIRS // CHUNKS
    pieces = [pltpu.make_async_copy(weights.at[pl.ds(i * per, per)], w.at[pl.ds(i * per, per)], wsem.at[i])
              for i in range(CHUNKS)]
    for cp in pieces:
        cp.start()
    acc[...] = jnp.zeros_like(acc)
    load.wait()
    step = 8
    for i in range(CHUNKS):
        pieces[i].wait()

        @pl.loop(0, per // step)
        def _(j):
            base = i * per + j * step
            prods = []
            for u in range(step):
                prods.append(jnp.dot(x[slot_ref[base + u]], w[base + u], preferred_element_type=jnp.float32))
            for u in range(step):
                t = target_ref[base + u]
                acc[t] = acc[t] + prods[u]

    total = jnp.zeros((VREG, BLK), jnp.float32)
    for t in range(TB):
        v = acc[t]
        total = total + v * area_ref[pl.ds(t, 1), :]
        out_ref[:, t * BLK:(t + 1) * BLK] = v
    mass_ref[...] = total


def regrid(pair_slot, pair_target, inb, weights, tgt_area):
    smem = pl.BlockSpec(memory_space=pltpu.SMEM)
    vmem = pl.BlockSpec(memory_space=pltpu.VMEM)
    hbm = pl.BlockSpec(memory_space=pl.ANY)
    return pl.pallas_call(
        regrid_kernel,
        out_shape=[jax.ShapeDtypeStruct((VREG, TB * BLK), jnp.float32), jax.ShapeDtypeStruct((VREG, BLK), jnp.float32)],
        in_specs=[smem, smem, hbm, hbm, vmem],
        out_specs=[vmem, vmem],
        scratch_shapes=[
            pltpu.VMEM((PEERS * CAP, VREG, BLK), jnp.bfloat16),
            pltpu.VMEM((PAIRS, BLK, BLK), jnp.bfloat16),
            pltpu.VMEM((TB, VREG, BLK), jnp.float32),
            pltpu.SemaphoreType.DMA,
            pltpu.SemaphoreType.DMA((CHUNKS,)),
        ],
        compiler_params=pltpu.CompilerParams(vmem_limit_bytes=40 * 2**20),
        name="regrid",
    )(pair_slot, pair_target, inb, weights, tgt_area)


def shards(src_field, src_area, tgt_area, weights, send_index, pair_slot, pair_target):
    inb = exchange(send_index[0].T, src_field)
    source_local = jnp.sum(src_field.astype(jnp.float32) * src_area[None, :], axis=1)
    regridded, partial = regrid(pair_slot, pair_target, inb.reshape(PEERS * CAP, VREG, BLK), weights,
                                tgt_area.reshape(TB, BLK))
    masses = lax.psum(jnp.stack([source_local, jnp.sum(partial, axis=1)]), AXES)
    return regridded * (masses[0] / masses[1])[:, None]


def solution(mesh):
    placed = (P(None, AXES), P(AXES), P(AXES), P(AXES, None, None), P(AXES, None, None), P(AXES), P(AXES))
    return jax.shard_map(shards, mesh=mesh, in_specs=placed, out_specs=P(None, AXES), check_vma=False)
```

```python
import itertools
import random

import jax
import jax.numpy as jnp
from jax import lax
from jax.experimental import pallas as pl
from jax.experimental.pallas import tpu as pltpu
from jax.sharding import PartitionSpec as P

AXES = ("row", "col")
MESH = pl.DeviceIdType.MESH
PEERS = 128
CAP = 2
BLK = 128
VREG = 64
SB = 256
TB = 64
PAIRS = 384
CHUNKS = 8


def offsets_in_order():
    every = [o for o in itertools.product(range(4), range(4), range(4), range(2)) if any(o)]

    def canon(o):
        forms = [tuple((s * v) % 4 for v in o[p:3] + o[:p]) for p in range(3) for s in (1, -1)]
        return min(forms) + o[3:]

    sets = {}
    for o in every:
        sets.setdefault(canon(o), []).append(o)
    rng = random.Random(5)
    groups = list(sets.values())
    rng.shuffle(groups)
    for g in groups:
        rng.shuffle(g)
    flat = [o for g in groups for o in g]
    return sorted(flat, key=lambda o: sum(v != 0 for v in o))


ORDER = offsets_in_order()
NEAR = [o for o in ORDER if sum(v != 0 for v in o) == 1]
PLANE = [o for o in ORDER if o[2] == 0 and o[3] == 0]


INDEX = {o: i for i, o in enumerate(ORDER)}
OPPOSITE = [INDEX[tuple((4 - v) % 4 for v in o[:3]) + o[3:]] for o in ORDER]
OTHERS = PEERS - 1
FIRST, SECOND = 80, 112


def split3(v):
    hi = v.astype(jnp.bfloat16)
    rest = v - hi.astype(jnp.float32)
    mid = rest.astype(jnp.bfloat16)
    return hi, mid, (rest - mid.astype(jnp.float32)).astype(jnp.bfloat16)


def exchange_kernel(send_ref, target_ref, slot_ref, src_area_ref, tgt_area_ref, src_hbm, weights, inb, ratio_ref,
                    src, outb, w, area3, upair, uout, uin, mout, min_, load_sem, self_sem, wsem, ssem, rsem,
                    usend, urecv, msend, mrecv, round_sem):
    row, col = lax.axis_index("row"), lax.axis_index("col")
    me = row * 16 + col
    z, k, y, x = row // 2, lax.rem(row, 2), col // 4, lax.rem(col, 4)

    def peer(o):
        dx, dy, dz, dk = o
        r = lax.rem(z + dz, 4) * 2 + lax.rem(k + dk, 2)
        c = lax.rem(y + dy, 4) * 4 + lax.rem(x + dx, 4)
        return r, c

    def load(b):
        return pltpu.make_async_copy(src_hbm.at[:, pl.ds(pl.multiple_of(b * BLK, BLK), BLK)], src.at[b], load_sem)

    barrier = pltpu.get_barrier_semaphore()
    for o in NEAR:
        pl.semaphore_signal(barrier, inc=1, device_id=peer(o), device_id_type=MESH)

    @pl.loop(0, SB, unroll=8)
    def _(b):
        load(b).start()

    per = PAIRS // CHUNKS
    pieces = [pltpu.make_async_copy(weights.at[pl.ds(i * per, per)], w.at[pl.ds(i * per, per)], wsem.at[i])
              for i in range(CHUNKS)]
    for cp in pieces:
        cp.start()

    rows = lax.broadcasted_iota(jnp.int32, (16, BLK), 0)

    @pl.loop(0, TB)
    def _(t):
        hi, mid, lo = (p.astype(jnp.float32) for p in split3(tgt_area_ref[pl.ds(t, 1), :]))
        stacked = jnp.where(rows == 0, hi, jnp.where(rows == 1, mid, jnp.where(rows == 2, lo, 0.0)))
        area3[t] = stacked.astype(jnp.bfloat16)

    @pl.loop(0, SB, unroll=8)
    def _(b):
        load(b).wait()

    def stage(i, dest):
        for c in range(CAP):
            block = jnp.maximum(send_ref[c, dest], 0)
            outb[i, c] = src[block]

    copies = []

    def send(lo, hi):
        for i in range(lo, hi):
            r, c = peer(ORDER[i])
            cp = pltpu.make_async_remote_copy(
                src_ref=outb.at[i], dst_ref=inb.at[me], send_sem=ssem.at[i], recv_sem=rsem.at[i],
                device_id=(r, c), device_id_type=MESH)
            cp.start()
            copies.append(cp)

    def stage_all(lo, hi):
        for i in range(lo, hi):
            r, c = peer(ORDER[i])
            stage(i, r * 16 + c)

    stage_all(0, 10)
    pl.semaphore_wait(barrier, len(NEAR))
    for o in NEAR:
        pl.semaphore_signal(round_sem.at[0], inc=1, device_id=peer(o), device_id_type=MESH)
    send(0, 10)
    stage_all(10, 46)
    pl.semaphore_wait(round_sem.at[0], len(NEAR))
    for o in PLANE:
        pl.semaphore_signal(round_sem.at[1], inc=1, device_id=peer(o), device_id_type=MESH)
    send(10, 46)
    stage_all(46, OTHERS)
    stage(OTHERS, me)
    own = pltpu.make_async_copy(outb.at[OTHERS], inb.at[me], self_sem)
    own.start()
    pl.semaphore_wait(round_sem.at[1], len(PLANE))
    send(46, FIRST)

    step = 8
    for i in range(CHUNKS):
        pieces[i].wait()

        @pl.loop(0, per // step)
        def _(j):
            base = i * per + j * step
            sums = []
            for u in range(step):
                r = lax.dot_general(area3[target_ref[base + u]], w[base + u], (((1,), (1,)), ((), ())),
                                    preferred_element_type=jnp.float32)
                sums.append(jnp.sum(r[0:8], axis=0, keepdims=True))
            upair[pl.ds(pl.multiple_of(base, step), step), :] = jnp.concatenate(sums, axis=0)

    parts = split3(upair[...])
    which = lax.broadcasted_iota(jnp.int32, (PEERS, PAIRS), 0) * CAP
    for c in range(CAP):
        chosen = jnp.where(slot_ref[...] == which + c, 1.0, 0.0).astype(jnp.bfloat16)
        total = sum(jnp.dot(chosen, p, preferred_element_type=jnp.float32) for p in parts)
        for d in range(PEERS):
            uout[d, :, c * BLK:(c + 1) * BLK] = total[d:d + 1, :]

    def source_mass(b, total):
        return total + src[b].astype(jnp.float32) * src_area_ref[pl.ds(b, 1), :]

    mass_s = lax.fori_loop(0, SB, source_mass, jnp.zeros((VREG, BLK), jnp.float32), unroll=4)

    for i in range(OTHERS):
        r, c = peer(ORDER[i])
        pltpu.make_async_remote_copy(
            src_ref=uout.at[r * 16 + c], dst_ref=uin.at[OPPOSITE[i]], send_sem=usend, recv_sem=urecv,
            device_id=(r, c), device_id_type=MESH).start()
    send(FIRST, SECOND)

    def weighed(blocks, u, total):
        for c in range(CAP):
            total = total + blocks[c].astype(jnp.float32) * u[:, c * BLK:(c + 1) * BLK]
        return total

    mass_t = weighed(outb.at[OTHERS], uout[me], jnp.zeros((VREG, BLK), jnp.float32))
    pltpu.make_async_copy(uin, uin, urecv).wait()
    mass_t = lax.fori_loop(0, OTHERS, lambda i, total: weighed(outb.at[i], uin[i], total), mass_t)
    local = jnp.sum(jnp.concatenate([mass_s, mass_t], axis=0).T, axis=0, keepdims=True)
    mout[...] = local
    send(SECOND, SECOND + 4)
    for i in range(OTHERS):
        pltpu.make_async_remote_copy(
            src_ref=mout, dst_ref=min_.at[i], send_sem=msend, recv_sem=mrecv,
            device_id=peer(ORDER[i]), device_id_type=MESH).start()
    send(SECOND + 4, OTHERS)
    pltpu.make_async_copy(min_, min_, mrecv).wait()
    total = lax.fori_loop(0, OTHERS, lambda i, t: t + min_[i], local)
    ratio_ref[...] = total / pltpu.roll(total, VREG, 1)
    own.wait()
    for cp in copies:
        cp.wait_recv()
    for cp in copies:
        cp.wait_send()
    pltpu.make_async_copy(uin, uin, usend).wait()
    pltpu.make_async_copy(min_, min_, msend).wait()


def exchange(send_rows, pair_target, pair_slot, src_area, tgt_area, src_field, weights):
    smem = pl.BlockSpec(memory_space=pltpu.SMEM)
    vmem = pl.BlockSpec(memory_space=pltpu.VMEM)
    hbm = pl.BlockSpec(memory_space=pl.ANY)
    dma = pltpu.SemaphoreType.DMA
    return pl.pallas_call(
        exchange_kernel,
        out_shape=[jax.ShapeDtypeStruct((PEERS, CAP, VREG, BLK), jnp.bfloat16),
                   jax.ShapeDtypeStruct((1, BLK), jnp.float32)],
        in_specs=[smem, smem, vmem, vmem, vmem, hbm, hbm],
        out_specs=[hbm, vmem],
        scratch_shapes=[
            pltpu.VMEM((SB, VREG, BLK), jnp.bfloat16),
            pltpu.VMEM((PEERS, CAP, VREG, BLK), jnp.bfloat16),
            pltpu.VMEM((PAIRS, BLK, BLK), jnp.bfloat16),
            pltpu.VMEM((TB, 16, BLK), jnp.bfloat16),
            pltpu.VMEM((PAIRS, BLK), jnp.float32),
            pltpu.VMEM((PEERS, 1, CAP * BLK), jnp.float32),
            pltpu.VMEM((OTHERS, 1, CAP * BLK), jnp.float32),
            pltpu.VMEM((1, BLK), jnp.float32),
            pltpu.VMEM((OTHERS, 1, BLK), jnp.float32),
            dma, dma, dma((CHUNKS,)), dma((PEERS,)), dma((PEERS,)), dma, dma, dma, dma,
            pltpu.SemaphoreType.REGULAR((2,)),
        ],
        compiler_params=pltpu.CompilerParams(
            collective_id=0, has_side_effects=True, vmem_limit_bytes=60 * 2**20),
        name="exchange",
    )(send_rows, pair_target, pair_slot, src_area, tgt_area, src_field, weights)


def regrid_kernel(slot_ref, target_ref, inb, weights, ratio_ref, out_ref, x, w, acc, xsem, wsem):
    load = pltpu.make_async_copy(inb, x, xsem)
    load.start()
    per = PAIRS // CHUNKS
    pieces = [pltpu.make_async_copy(weights.at[pl.ds(i * per, per)], w.at[pl.ds(i * per, per)], wsem.at[i])
              for i in range(CHUNKS)]
    for cp in pieces:
        cp.start()
    acc[...] = jnp.zeros_like(acc)
    load.wait()
    step = 8
    for i in range(CHUNKS):
        pieces[i].wait()

        @pl.loop(0, per // step)
        def _(j):
            base = i * per + j * step
            prods = []
            for u in range(step):
                prods.append(jnp.dot(x[slot_ref[base + u]], w[base + u], preferred_element_type=jnp.float32))
            for u in range(step):
                t = target_ref[base + u]
                acc[t] = acc[t] + prods[u]

    ratio = jnp.broadcast_to(ratio_ref[...], (BLK, BLK)).T[:VREG]
    for t in range(TB):
        out_ref[:, t * BLK:(t + 1) * BLK] = acc[t] * ratio


def regrid(pair_slot, pair_target, inb, weights, ratio):
    smem = pl.BlockSpec(memory_space=pltpu.SMEM)
    vmem = pl.BlockSpec(memory_space=pltpu.VMEM)
    hbm = pl.BlockSpec(memory_space=pl.ANY)
    return pl.pallas_call(
        regrid_kernel,
        out_shape=jax.ShapeDtypeStruct((VREG, TB * BLK), jnp.float32),
        in_specs=[smem, smem, hbm, hbm, vmem],
        out_specs=vmem,
        scratch_shapes=[
            pltpu.VMEM((PEERS * CAP, VREG, BLK), jnp.bfloat16),
            pltpu.VMEM((PAIRS, BLK, BLK), jnp.bfloat16),
            pltpu.VMEM((TB, VREG, BLK), jnp.float32),
            pltpu.SemaphoreType.DMA,
            pltpu.SemaphoreType.DMA((CHUNKS,)),
        ],
        compiler_params=pltpu.CompilerParams(vmem_limit_bytes=60 * 2**20),
        name="regrid",
    )(pair_slot, pair_target, inb, weights, ratio)


def shards(src_field, src_area, tgt_area, weights, send_index, pair_slot, pair_target):
    inb, ratio = exchange(send_index[0].T, pair_target, pair_slot.reshape(1, PAIRS), src_area.reshape(SB, BLK),
                          tgt_area.reshape(TB, BLK), src_field, weights)
    return regrid(pair_slot, pair_target, inb.reshape(PEERS * CAP, VREG, BLK), weights, ratio)


def solution(mesh):
    placed = (P(None, AXES), P(AXES), P(AXES), P(AXES, None, None), P(AXES, None, None), P(AXES), P(AXES))
    return jax.shard_map(shards, mesh=mesh, in_specs=placed, out_specs=P(None, AXES), check_vma=False)
```

```python
import itertools
import random

import jax
import jax.numpy as jnp
from jax import lax
from jax.experimental import pallas as pl
from jax.experimental.pallas import tpu as pltpu
from jax.sharding import PartitionSpec as P

AXES = ("row", "col")
MESH = pl.DeviceIdType.MESH
PEERS = 128
CAP = 2
BLK = 128
VREG = 64
SB = 256
TB = 64
PAIRS = 384
CHUNKS = 8


def offsets_in_order():
    every = [o for o in itertools.product(range(4), range(4), range(4), range(2)) if any(o)]

    def canon(o):
        forms = [tuple((s * v) % 4 for v in o[p:3] + o[:p]) for p in range(3) for s in (1, -1)]
        return min(forms) + o[3:]

    sets = {}
    for o in every:
        sets.setdefault(canon(o), []).append(o)
    rng = random.Random(5)
    groups = list(sets.values())
    rng.shuffle(groups)
    for g in groups:
        rng.shuffle(g)
    flat = [o for g in groups for o in g]
    return sorted(flat, key=lambda o: (sum(v != 0 for v in o), group_of(o)))


def group_of(o):
    differing = sum(v != 0 for v in o)
    if differing <= 2:
        return 0
    if differing == 3:
        return 1 + o[3]
    return 3 if sum(o[:3]) % 3 else 4


ORDER = offsets_in_order()
GROUPS = 5
ENDS = [sum(group_of(o) <= g for o in ORDER) for g in range(GROUPS)]
FIRST = 90
ROOM = (160, 96, 96, 80)
NEAR = [o for o in ORDER if sum(v != 0 for v in o) == 1]
PLANE = [o for o in ORDER if o[2] == 0 and o[3] == 0]


INDEX = {o: i for i, o in enumerate(ORDER)}
OPPOSITE = [INDEX[tuple((4 - v) % 4 for v in o[:3]) + o[3:]] for o in ORDER]
OTHERS = PEERS - 1
PER = PAIRS // CHUNKS


def split3(v):
    hi = v.astype(jnp.bfloat16)
    rest = v - hi.astype(jnp.float32)
    mid = rest.astype(jnp.bfloat16)
    return hi, mid, (rest - mid.astype(jnp.float32)).astype(jnp.bfloat16)


def columns(row):
    parts = [jnp.broadcast_to(row[:, c:c + BLK], (BLK, BLK)).T for c in range(0, PAIRS, BLK)]
    return jnp.concatenate(parts, axis=0)


def add_rows(m):
    acc = m[0:8]
    for i in range(8, PAIRS, 8):
        acc = acc + m[i:i + 8]
    for shift in (4, 2, 1):
        acc = acc + pltpu.roll(acc, shift, 0)
    return acc[0:1]


def pair_table(slot, target, z, k, y, x):
    sender = lax.shift_right_logical(slot, 1)
    dz = (z - lax.shift_right_logical(sender, 5) + 4) & 3
    dk = (k - lax.shift_right_logical(sender, 4)) & 1
    dy = (y - lax.shift_right_logical(sender, 2)) & 3
    dx = (x - sender) & 3
    differing = sum(jnp.where(v != 0, 1, 0) for v in (dx, dy, dz, dk))
    steps = dx + dy + dz
    last = jnp.where((steps == 3) | (steps == 6) | (steps == 9), 4, 3)
    group = jnp.where(differing <= 2, 0, jnp.where(differing == 3, 1 + dk, last))
    lane = lax.broadcasted_iota(jnp.int32, (1, PAIRS), 1)
    key = (group * TB + target) * 512 + lane
    key_col = columns(key)
    rank = jnp.concatenate([add_rows(jnp.where(key_col < key[:, c:c + BLK], 1, 0)) for c in range(0, PAIRS, BLK)], axis=1)
    packed_col = columns(lane * 16384 + slot * 64 + target)
    rank_col = columns(rank)
    lanes = lax.broadcasted_iota(jnp.int32, (PAIRS, BLK), 1)
    packed = [add_rows(jnp.where(rank_col == lanes + c, packed_col, 0)) for c in range(0, PAIRS, BLK)]
    upto = [add_rows(jnp.where(key_col < (lanes + (c + 1)) * 512, 1, 0)) for c in range(0, PAIRS, BLK)]
    return jnp.concatenate(packed, axis=1), jnp.concatenate(upto, axis=1)


def exchange_kernel(send_ref, target_ref, slots_ref, targets_ref, src_area_ref, tgt_area_ref, src_hbm, weights,
                    inb, partial, table_ref, ratio_ref,
                    src, outb, w, xa, xb, prods, acc, area3, upair, uout, uin, mout, min_, table,
                    load_sem, self_sem, wsem, ssem, rsem, usend, urecv, msend, mrecv, tsem, xsem, psem, round_sem):
    row, col = lax.axis_index("row"), lax.axis_index("col")
    me = row * 16 + col
    z, k, y, x_ = row // 2, lax.rem(row, 2), col // 4, lax.rem(col, 4)

    def peer(o, sign=1):
        dx, dy, dz, dk = o
        r = lax.rem(z + sign * dz + 4, 4) * 2 + lax.rem(k + dk, 2)
        c = lax.rem(y + sign * dy + 4, 4) * 4 + lax.rem(x_ + sign * dx + 4, 4)
        return r, c

    def load(b):
        return pltpu.make_async_copy(src_hbm.at[:, pl.ds(pl.multiple_of(b * BLK, BLK), BLK)], src.at[b], load_sem)

    xs = (xa, xb)
    barrier = pltpu.get_barrier_semaphore()
    for o in NEAR:
        pl.semaphore_signal(barrier, inc=1, device_id=peer(o), device_id_type=MESH)
    pieces = [pltpu.make_async_copy(weights.at[pl.ds(i * PER, PER)], w.at[pl.ds(i * PER, PER)], wsem.at[i])
              for i in range(CHUNKS)]

    @pl.loop(0, SB, unroll=8)
    def _(b):
        load(b).start()

    step = 16

    def weight_sums(i):
        pieces[i].wait()

        @pl.loop(0, PER // step)
        def _(j):
            base = i * PER + j * step
            sums = []
            for u in range(step):
                r = lax.dot_general(area3[target_ref[base + u]], w[base + u], (((1,), (1,)), ((), ())),
                                    preferred_element_type=jnp.float32)
                sums.append(jnp.sum(r[0:8], axis=0, keepdims=True))
            upair[pl.ds(pl.multiple_of(base, step), step), :] = jnp.concatenate(sums, axis=0)

    def stage(lo, hi):
        for i in range(lo, hi):
            if i < OTHERS:
                r, c = peer(ORDER[i])
                dest = r * 16 + c
            else:
                dest = me
            for c in range(CAP):
                outb[i, c] = src[jnp.maximum(send_ref[c, dest], 0)]

    copies = []

    def send(lo, hi):
        for i in range(lo, hi):
            r, c = peer(ORDER[i])
            cp = pltpu.make_async_remote_copy(
                src_ref=outb.at[i], dst_ref=inb.at[me], send_sem=ssem.at[i], recv_sem=rsem.at[i],
                device_id=(r, c), device_id_type=MESH)
            cp.start()
            copies.append(cp)

    def fetch(g, with_own=False):
        lo, hi, x = ENDS[g - 1] if g else 0, ENDS[g], xs[g % 2]
        local = []
        for i in range(lo, hi):
            copies[i].wait_recv()
            r, c = peer(ORDER[i], -1)
            s = r * 16 + c
            local.append(pltpu.make_async_copy(inb.at[s], x.at[pl.ds(s * CAP, CAP)], xsem.at[i]))
            local[-1].start()
        if with_own:
            own.wait()
            local.append(pltpu.make_async_copy(inb.at[me], x.at[pl.ds(me * CAP, CAP)], xsem.at[OTHERS]))
            local[-1].start()
        return local

    def regrid_group(g, local):
        room, x = ROOM[g], xs[g % 2]
        for cp in local:
            cp.wait()
        start = table[1, g * TB - 1] if g else 0

        def some(n, carry):
            total, before = carry
            for u in range(step):
                entry = table[0, jnp.minimum(start + n * step + u, PAIRS - 1)]
                t = entry & 63
                product = jnp.dot(x[lax.shift_right_logical(entry, 6) & 255], w[lax.shift_right_logical(entry, 14)],
                                  preferred_element_type=jnp.float32)
                total = total * jnp.where(t == before, 1.0, 0.0) + product
                before = t
                prods[n * step + u] = total
            return total, before

        lax.fori_loop(0, room // step, some, (jnp.zeros((VREG, BLK), jnp.float32), jnp.int32(-1)))

        @pl.loop(0, TB)
        def _(t):
            end = table[1, g * TB + t]
            begin = table[1, jnp.maximum(g * TB + t - 1, 0)]
            if g == 0:
                begin = jnp.where(t == 0, 0, begin)
            there = (end > begin) & (begin - start < room)
            v = prods[jnp.clip(end - 1 - start, 0, room - 1)]
            v = jnp.where(there, v, 0.0)
            acc[t] = v if g == 0 else acc[t] + v


    @pl.loop(0, SB, unroll=8)
    def _(b):
        load(b).wait()

    for cp in pieces:
        cp.start()
    stage(0, 10)
    pl.semaphore_wait(barrier, len(NEAR))
    for o in NEAR:
        pl.semaphore_signal(round_sem.at[0], inc=1, device_id=peer(o), device_id_type=MESH)
    send(0, 10)
    stage(10, 46)
    rows = lax.broadcasted_iota(jnp.int32, (16, BLK), 0)

    @pl.loop(0, TB)
    def _(t):
        hi, mid, lo = (p.astype(jnp.float32) for p in split3(tgt_area_ref[pl.ds(t, 1), :]))
        stacked = jnp.where(rows == 0, hi, jnp.where(rows == 1, mid, jnp.where(rows == 2, lo, 0.0)))
        area3[t] = stacked.astype(jnp.bfloat16)

    weight_sums(0)
    pl.semaphore_wait(round_sem.at[0], len(NEAR))
    for o in PLANE:
        pl.semaphore_signal(round_sem.at[1], inc=1, device_id=peer(o), device_id_type=MESH)
    send(10, 46)
    stage(46, PEERS)
    own = pltpu.make_async_copy(outb.at[OTHERS], inb.at[me], self_sem)
    own.start()
    weight_sums(1)
    weight_sums(2)
    pl.semaphore_wait(round_sem.at[1], len(PLANE))
    send(46, FIRST)
    for i in range(3, 8):
        weight_sums(i)

    parts = split3(upair[...])
    slots = slots_ref[...].reshape(1, PAIRS)
    which = lax.broadcasted_iota(jnp.int32, (PEERS, PAIRS), 0) * CAP
    for c in range(CAP):
        chosen = jnp.where(slots == which + c, 1.0, 0.0).astype(jnp.bfloat16)
        total = sum(jnp.dot(chosen, p, preferred_element_type=jnp.float32) for p in parts)
        for d in range(PEERS):
            uout[d, :, c * BLK:(c + 1) * BLK] = total[d:d + 1, :]

    for i in range(OTHERS):
        r, c = peer(ORDER[i])
        pltpu.make_async_remote_copy(
            src_ref=uout.at[r * 16 + c], dst_ref=uin.at[OPPOSITE[i]], send_sem=usend, recv_sem=urecv,
            device_id=(r, c), device_id_type=MESH).start()
    send(FIRST, OTHERS)
    packed, upto = pair_table(slots, targets_ref[...].reshape(1, PAIRS), z, k, y, x_)
    table_ref[0:1, :] = packed
    table_ref[1:2, :] = upto

    def source_mass(b, total):
        return total + src[b].astype(jnp.float32) * src_area_ref[pl.ds(b, 1), :]

    scalars = pltpu.make_async_copy(table_ref, table, tsem)
    scalars.start()
    local = fetch(0, with_own=True)
    mass_s = lax.fori_loop(0, SB, source_mass, jnp.zeros((VREG, BLK), jnp.float32), unroll=4)
    scalars.wait()
    regrid_group(0, local)
    local = fetch(1)

    def weighed(blocks, u, total):
        for c in range(CAP):
            total = total + blocks[c].astype(jnp.float32) * u[:, c * BLK:(c + 1) * BLK]
        return total

    mass_t = weighed(outb.at[OTHERS], uout[me], jnp.zeros((VREG, BLK), jnp.float32))
    pltpu.make_async_copy(uin, uin, urecv).wait()
    mass_t = lax.fori_loop(0, OTHERS, lambda i, total: weighed(outb.at[i], uin[i], total), mass_t)
    sums = jnp.sum(jnp.concatenate([mass_s, mass_t], axis=0).T, axis=0, keepdims=True)
    mout[...] = sums
    for i in range(OTHERS):
        pltpu.make_async_remote_copy(
            src_ref=mout, dst_ref=min_.at[i], send_sem=msend, recv_sem=mrecv,
            device_id=peer(ORDER[i]), device_id_type=MESH).start()
    for g in range(1, GROUPS - 1):
        regrid_group(g, local)
        if g < GROUPS - 2:
            local = fetch(g + 1)
    out = pltpu.make_async_copy(acc, partial, psem)
    out.start()
    pltpu.make_async_copy(min_, min_, mrecv).wait()
    total = lax.fori_loop(0, OTHERS, lambda i, t: t + min_[i], sums)
    ratio_ref[...] = total / pltpu.roll(total, VREG, 1)
    for i in range(ENDS[3], OTHERS):
        copies[i].wait_recv()
    for cp in copies:
        cp.wait_send()
    pltpu.make_async_copy(uin, uin, usend).wait()
    pltpu.make_async_copy(min_, min_, msend).wait()
    out.wait()


def exchange(send_rows, pair_target, pair_slot, src_area, tgt_area, src_field, weights):
    smem = pl.BlockSpec(memory_space=pltpu.SMEM)
    vmem = pl.BlockSpec(memory_space=pltpu.VMEM)
    hbm = pl.BlockSpec(memory_space=pl.ANY)
    dma = pltpu.SemaphoreType.DMA
    return pl.pallas_call(
        exchange_kernel,
        out_shape=[jax.ShapeDtypeStruct((PEERS, CAP, VREG, BLK), jnp.bfloat16),
                   jax.ShapeDtypeStruct((TB, VREG, BLK), jnp.float32),
                   jax.ShapeDtypeStruct((8, PAIRS), jnp.int32),
                   jax.ShapeDtypeStruct((1, BLK), jnp.float32)],
        in_specs=[smem, smem, vmem, vmem, vmem, vmem, hbm, hbm],
        out_specs=[hbm, hbm, vmem, vmem],
        scratch_shapes=[
            pltpu.VMEM((SB, VREG, BLK), jnp.bfloat16),
            pltpu.VMEM((PEERS, CAP, VREG, BLK), jnp.bfloat16),
            pltpu.VMEM((PAIRS, BLK, BLK), jnp.bfloat16),
            pltpu.VMEM((PEERS * CAP, VREG, BLK), jnp.bfloat16),
            pltpu.VMEM((PEERS * CAP, VREG, BLK), jnp.bfloat16),
            pltpu.VMEM((max(ROOM), VREG, BLK), jnp.float32),
            pltpu.VMEM((TB, VREG, BLK), jnp.float32),
            pltpu.VMEM((TB, 16, BLK), jnp.bfloat16),
            pltpu.VMEM((PAIRS, BLK), jnp.float32),
            pltpu.VMEM((PEERS, 1, CAP * BLK), jnp.float32),
            pltpu.VMEM((OTHERS, 1, CAP * BLK), jnp.float32),
            pltpu.VMEM((1, BLK), jnp.float32),
            pltpu.VMEM((OTHERS, 1, BLK), jnp.float32),
            pltpu.SMEM((8, PAIRS), jnp.int32),
            dma, dma, dma((CHUNKS,)), dma((PEERS,)), dma((PEERS,)), dma, dma, dma, dma, dma, dma((PEERS,)), dma,
            pltpu.SemaphoreType.REGULAR((2,)),
        ],
        compiler_params=pltpu.CompilerParams(
            collective_id=0, has_side_effects=True, vmem_limit_bytes=60 * 2**20),
        name="exchange",
    )(send_rows, pair_target, pair_slot, pair_target, src_area, tgt_area, src_field, weights)


HELD = 32


def finish_kernel(table, inb, weights, partial, ratio_ref, out, x, w, acc, scaled, xsem, wsem, asem, osem):
    load = pltpu.make_async_copy(partial, acc, asem)
    load.start()
    ranges = [(jnp.where(g == 0, 0, table[1, max(g * TB - 1, 0)]) + (ROOM[g] if g < GROUPS - 1 else 0),
               table[1, g * TB + TB - 1]) for g in range(GROUPS)]
    step = 8

    def copies(j, u):
        entry = table[0, j]
        slot = lax.shift_right_logical(entry, 6) & 255
        return (pltpu.make_async_copy(inb.at[slot], x.at[u], xsem),
                pltpu.make_async_copy(weights.at[lax.shift_right_logical(entry, 14)], w.at[u], wsem))

    def bring(lo, count):
        def one(u, _):
            for cp in copies(lo + u, u):
                cp.start()
            return 0

        lax.fori_loop(0, count, one, 0)

    def use(lo, count):
        def one(u, _):
            for cp in copies(lo + u, u):
                cp.wait()
            return 0

        lax.fori_loop(0, count, one, 0)

        def some(n, _):
            products = [jnp.dot(x[n * step + u], w[n * step + u], preferred_element_type=jnp.float32)
                        for u in range(step)]
            for u in range(step):
                i = n * step + u
                t = table[0, jnp.minimum(lo + i, PAIRS - 1)] & 63
                acc[t] = acc[t] + jnp.where(i < count, products[u], 0.0)
            return 0

        lax.fori_loop(0, lax.div(count + step - 1, step), some, 0)

    lo, hi = ranges[-1]
    count = jnp.minimum(hi - lo, HELD)
    bring(lo, count)
    ratio = jnp.broadcast_to(ratio_ref[...], (BLK, BLK)).T[:VREG]
    load.wait()
    use(lo, count)
    ranges[-1] = (lo + count, hi)
    for lo, hi in ranges:
        def more(n, _, lo=lo, hi=hi):
            first = lo + n * HELD
            count = jnp.minimum(hi - first, HELD)
            bring(first, count)
            use(first, count)
            return 0

        lax.fori_loop(0, lax.div(jnp.maximum(hi - lo, 0) + HELD - 1, HELD), more, 0)

    parts = 4
    per = TB // parts
    done = []
    for i in range(parts):
        for t in range(i * per, (i + 1) * per):
            scaled[:, t * BLK:(t + 1) * BLK] = acc[t] * ratio
        span = pl.ds(i * per * BLK, per * BLK)
        done.append(pltpu.make_async_copy(scaled.at[:, span], out.at[:, span], osem.at[i]))
        done[-1].start()
    for cp in done:
        cp.wait()


def finish(table, inb, weights, partial, ratio):
    smem = pl.BlockSpec(memory_space=pltpu.SMEM)
    vmem = pl.BlockSpec(memory_space=pltpu.VMEM)
    hbm = pl.BlockSpec(memory_space=pl.ANY)
    dma = pltpu.SemaphoreType.DMA
    return pl.pallas_call(
        finish_kernel,
        out_shape=jax.ShapeDtypeStruct((VREG, TB * BLK), jnp.float32),
        in_specs=[smem, hbm, hbm, hbm, vmem],
        out_specs=hbm,
        scratch_shapes=[
            pltpu.VMEM((HELD, VREG, BLK), jnp.bfloat16),
            pltpu.VMEM((HELD, BLK, BLK), jnp.bfloat16),
            pltpu.VMEM((TB, VREG, BLK), jnp.float32),
            pltpu.VMEM((VREG, TB * BLK), jnp.float32),
            dma, dma, dma, dma((4,)),
        ],
        compiler_params=pltpu.CompilerParams(vmem_limit_bytes=60 * 2**20),
        name="finish",
    )(table, inb, weights, partial, ratio)


def shards(src_field, src_area, tgt_area, weights, send_index, pair_slot, pair_target):
    inb, partial, table, ratio = exchange(
        send_index[0].T, pair_target, pair_slot, src_area.reshape(SB, BLK), tgt_area.reshape(TB, BLK), src_field, weights)
    return finish(table, inb.reshape(PEERS * CAP, VREG, BLK), weights, partial, ratio)


def solution(mesh):
    placed = (P(None, AXES), P(AXES), P(AXES), P(AXES, None, None), P(AXES, None, None), P(AXES), P(AXES))
    return jax.shard_map(shards, mesh=mesh, in_specs=placed, out_specs=P(None, AXES), check_vma=False)
```

```python
import itertools
import random

import jax
import jax.numpy as jnp
from jax import lax
from jax.experimental import pallas as pl
from jax.experimental.pallas import tpu as pltpu
from jax.sharding import PartitionSpec as P

AXES = ("row", "col")
MESH = pl.DeviceIdType.MESH
PEERS = 128
CAP = 2
BLK = 128
VREG = 64
SB = 256
TB = 64
PAIRS = 384
CHUNKS = 8


def offsets_in_order():
    every = [o for o in itertools.product(range(4), range(4), range(4), range(2)) if any(o)]

    def canon(o):
        forms = [tuple((s * v) % 4 for v in o[p:3] + o[:p]) for p in range(3) for s in (1, -1)]
        return min(forms) + o[3:]

    sets = {}
    for o in every:
        sets.setdefault(canon(o), []).append(o)
    rng = random.Random(5)
    groups = list(sets.values())
    rng.shuffle(groups)
    for g in groups:
        rng.shuffle(g)
    flat = [o for g in groups for o in g]
    return sorted(flat, key=lambda o: (sum(v != 0 for v in o), group_of(o)))


def group_of(o):
    differing = sum(v != 0 for v in o)
    if differing <= 2:
        return 0
    if differing == 3:
        return 1 + o[3]
    return 3 if sum(o[:3]) % 3 else 4


ORDER = offsets_in_order()
GROUPS = 5
ENDS = [sum(group_of(o) <= g for o in ORDER) for g in range(GROUPS)]
FIRST = 86
ROOM = (160, 96, 96, 80)
NEAR = [o for o in ORDER if sum(v != 0 for v in o) == 1]
PLANE = [o for o in ORDER if o[2] == 0 and o[3] == 0]


INDEX = {o: i for i, o in enumerate(ORDER)}
OPPOSITE = [INDEX[tuple((4 - v) % 4 for v in o[:3]) + o[3:]] for o in ORDER]
OTHERS = PEERS - 1
PER = PAIRS // CHUNKS


def split3(v):
    hi = v.astype(jnp.bfloat16)
    rest = v - hi.astype(jnp.float32)
    mid = rest.astype(jnp.bfloat16)
    return hi, mid, (rest - mid.astype(jnp.float32)).astype(jnp.bfloat16)


def columns(row):
    parts = [jnp.broadcast_to(row[:, c:c + BLK], (BLK, BLK)).T for c in range(0, PAIRS, BLK)]
    return jnp.concatenate(parts, axis=0)


def add_rows(m):
    acc = m[0:8]
    for i in range(8, PAIRS, 8):
        acc = acc + m[i:i + 8]
    for shift in (4, 2, 1):
        acc = acc + pltpu.roll(acc, shift, 0)
    return acc[0:1]


def pair_table(slot, target, z, k, y, x):
    sender = lax.shift_right_logical(slot, 1)
    dz = (z - lax.shift_right_logical(sender, 5) + 4) & 3
    dk = (k - lax.shift_right_logical(sender, 4)) & 1
    dy = (y - lax.shift_right_logical(sender, 2)) & 3
    dx = (x - sender) & 3
    differing = sum(jnp.where(v != 0, 1, 0) for v in (dx, dy, dz, dk))
    steps = dx + dy + dz
    last = jnp.where((steps == 3) | (steps == 6) | (steps == 9), 4, 3)
    group = jnp.where(differing <= 2, 0, jnp.where(differing == 3, 1 + dk, last))
    lane = lax.broadcasted_iota(jnp.int32, (1, PAIRS), 1)
    key = (group * TB + target) * 512 + lane
    key_col = columns(key)
    rank = jnp.concatenate([add_rows(jnp.where(key_col < key[:, c:c + BLK], 1, 0)) for c in range(0, PAIRS, BLK)], axis=1)
    packed_col = columns(lane * 16384 + slot * 64 + target)
    rank_col = columns(rank)
    lanes = lax.broadcasted_iota(jnp.int32, (PAIRS, BLK), 1)
    packed = [add_rows(jnp.where(rank_col == lanes + c, packed_col, 0)) for c in range(0, PAIRS, BLK)]
    upto = [add_rows(jnp.where(key_col < (lanes + (c + 1)) * 512, 1, 0)) for c in range(0, PAIRS, BLK)]
    return jnp.concatenate(packed, axis=1), jnp.concatenate(upto, axis=1)


def exchange_kernel(send_ref, target_ref, slots_ref, targets_ref, src_area_ref, tgt_area_ref, src_hbm, weights,
                    inb, partial, table_ref, ratio_ref,
                    src, outb, w, xa, xb, prods, acc, area3, upair, uout, uin, mout, min_, table,
                    load_sem, self_sem, wsem, ssem, rsem, usend, urecv, msend, mrecv, tsem, xsem, psem, round_sem):
    row, col = lax.axis_index("row"), lax.axis_index("col")
    me = row * 16 + col
    z, k, y, x_ = row // 2, lax.rem(row, 2), col // 4, lax.rem(col, 4)

    def peer(o, sign=1):
        dx, dy, dz, dk = o
        r = lax.rem(z + sign * dz + 4, 4) * 2 + lax.rem(k + dk, 2)
        c = lax.rem(y + sign * dy + 4, 4) * 4 + lax.rem(x_ + sign * dx + 4, 4)
        return r, c

    def load(b):
        return pltpu.make_async_copy(src_hbm.at[:, pl.ds(pl.multiple_of(b * BLK, BLK), BLK)], src.at[b], load_sem)

    xs = (xa, xb)
    barrier = pltpu.get_barrier_semaphore()
    for o in NEAR:
        pl.semaphore_signal(barrier, inc=1, device_id=peer(o), device_id_type=MESH)
    pieces = [pltpu.make_async_copy(weights.at[pl.ds(i * PER, PER)], w.at[pl.ds(i * PER, PER)], wsem.at[i])
              for i in range(CHUNKS)]

    @pl.loop(0, SB, unroll=8)
    def _(b):
        load(b).start()

    step = 16

    def weight_sums(i):
        pieces[i].wait()

        @pl.loop(0, PER // step)
        def _(j):
            base = i * PER + j * step
            sums = []
            for u in range(step):
                r = lax.dot_general(area3[target_ref[base + u]], w[base + u], (((1,), (1,)), ((), ())),
                                    preferred_element_type=jnp.float32)
                sums.append(jnp.sum(r[0:8], axis=0, keepdims=True))
            upair[pl.ds(pl.multiple_of(base, step), step), :] = jnp.concatenate(sums, axis=0)

    def stage(lo, hi):
        for i in range(lo, hi):
            if i < OTHERS:
                r, c = peer(ORDER[i])
                dest = r * 16 + c
            else:
                dest = me
            for c in range(CAP):
                outb[i, c] = src[jnp.maximum(send_ref[c, dest], 0)]

    copies = []

    def send(lo, hi):
        for i in range(lo, hi):
            r, c = peer(ORDER[i])
            cp = pltpu.make_async_remote_copy(
                src_ref=outb.at[i], dst_ref=inb.at[me], send_sem=ssem.at[i], recv_sem=rsem.at[i],
                device_id=(r, c), device_id_type=MESH)
            cp.start()
            copies.append(cp)

    def fetch(g, with_own=False):
        lo, hi, x = ENDS[g - 1] if g else 0, ENDS[g], xs[g % 2]
        local = []
        for i in range(lo, hi):
            copies[i].wait_recv()
            r, c = peer(ORDER[i], -1)
            s = r * 16 + c
            local.append(pltpu.make_async_copy(inb.at[s], x.at[pl.ds(s * CAP, CAP)], xsem.at[i]))
            local[-1].start()
        if with_own:
            own.wait()
            local.append(pltpu.make_async_copy(inb.at[me], x.at[pl.ds(me * CAP, CAP)], xsem.at[OTHERS]))
            local[-1].start()
        return local

    def regrid_group(g, local):
        room, x = ROOM[g], xs[g % 2]
        for cp in local:
            cp.wait()
        start = table[1, g * TB - 1] if g else 0

        def some(n, carry):
            total, before = carry
            for u in range(step):
                entry = table[0, jnp.minimum(start + n * step + u, PAIRS - 1)]
                t = entry & 63
                product = jnp.dot(x[lax.shift_right_logical(entry, 6) & 255], w[lax.shift_right_logical(entry, 14)],
                                  preferred_element_type=jnp.float32)
                total = total * jnp.where(t == before, 1.0, 0.0) + product
                before = t
                prods[n * step + u] = total
            return total, before

        lax.fori_loop(0, room // step, some, (jnp.zeros((VREG, BLK), jnp.float32), jnp.int32(-1)))

        @pl.loop(0, TB)
        def _(t):
            end = table[1, g * TB + t]
            begin = table[1, jnp.maximum(g * TB + t - 1, 0)]
            if g == 0:
                begin = jnp.where(t == 0, 0, begin)
            there = (end > begin) & (begin - start < room)
            v = prods[jnp.clip(end - 1 - start, 0, room - 1)]
            v = jnp.where(there, v, 0.0)
            acc[t] = v if g == 0 else acc[t] + v


    @pl.loop(0, SB, unroll=8)
    def _(b):
        load(b).wait()

    for cp in pieces:
        cp.start()
    stage(0, 10)
    pl.semaphore_wait(barrier, len(NEAR))
    for o in NEAR:
        pl.semaphore_signal(round_sem.at[0], inc=1, device_id=peer(o), device_id_type=MESH)
    send(0, 10)
    stage(10, 46)
    rows = lax.broadcasted_iota(jnp.int32, (16, BLK), 0)

    @pl.loop(0, TB)
    def _(t):
        hi, mid, lo = (p.astype(jnp.float32) for p in split3(tgt_area_ref[pl.ds(t, 1), :]))
        stacked = jnp.where(rows == 0, hi, jnp.where(rows == 1, mid, jnp.where(rows == 2, lo, 0.0)))
        area3[t] = stacked.astype(jnp.bfloat16)

    weight_sums(0)
    pl.semaphore_wait(round_sem.at[0], len(NEAR))
    for o in PLANE:
        pl.semaphore_signal(round_sem.at[1], inc=1, device_id=peer(o), device_id_type=MESH)
    send(10, 46)
    stage(46, PEERS)
    own = pltpu.make_async_copy(outb.at[OTHERS], inb.at[me], self_sem)
    own.start()
    weight_sums(1)
    weight_sums(2)
    pl.semaphore_wait(round_sem.at[1], len(PLANE))
    send(46, FIRST)
    for i in range(3, 8):
        weight_sums(i)

    parts = split3(upair[...])
    slots = slots_ref[...].reshape(1, PAIRS)
    which = lax.broadcasted_iota(jnp.int32, (PEERS, PAIRS), 0) * CAP
    for c in range(CAP):
        chosen = jnp.where(slots == which + c, 1.0, 0.0).astype(jnp.bfloat16)
        total = sum(jnp.dot(chosen, p, preferred_element_type=jnp.float32) for p in parts)
        for d in range(PEERS):
            uout[d, :, c * BLK:(c + 1) * BLK] = total[d:d + 1, :]

    for i in range(OTHERS):
        r, c = peer(ORDER[i])
        pltpu.make_async_remote_copy(
            src_ref=uout.at[r * 16 + c], dst_ref=uin.at[OPPOSITE[i]], send_sem=usend, recv_sem=urecv,
            device_id=(r, c), device_id_type=MESH).start()
    send(FIRST, OTHERS)
    packed, upto = pair_table(slots, targets_ref[...].reshape(1, PAIRS), z, k, y, x_)
    table_ref[0:1, :] = packed
    table_ref[1:2, :] = upto

    def source_mass(b, total):
        return total + src[b].astype(jnp.float32) * src_area_ref[pl.ds(b, 1), :]

    scalars = pltpu.make_async_copy(table_ref, table, tsem)
    scalars.start()
    local = fetch(0, with_own=True)
    mass_s = lax.fori_loop(0, SB, source_mass, jnp.zeros((VREG, BLK), jnp.float32), unroll=4)
    scalars.wait()
    regrid_group(0, local)
    local = fetch(1)

    def weighed(blocks, u, total):
        for c in range(CAP):
            total = total + blocks[c].astype(jnp.float32) * u[:, c * BLK:(c + 1) * BLK]
        return total

    mass_t = weighed(outb.at[OTHERS], uout[me], jnp.zeros((VREG, BLK), jnp.float32))
    pltpu.make_async_copy(uin, uin, urecv).wait()
    mass_t = lax.fori_loop(0, OTHERS, lambda i, total: weighed(outb.at[i], uin[i], total), mass_t)
    sums = jnp.sum(jnp.concatenate([mass_s, mass_t], axis=0).T, axis=0, keepdims=True)
    mout[...] = sums
    for i in range(OTHERS):
        pltpu.make_async_remote_copy(
            src_ref=mout, dst_ref=min_.at[i], send_sem=msend, recv_sem=mrecv,
            device_id=peer(ORDER[i]), device_id_type=MESH).start()
    for g in range(1, GROUPS - 1):
        regrid_group(g, local)
        if g < GROUPS - 2:
            local = fetch(g + 1)
    out = pltpu.make_async_copy(acc, partial, psem)
    out.start()
    pltpu.make_async_copy(min_, min_, mrecv).wait()
    total = lax.fori_loop(0, OTHERS, lambda i, t: t + min_[i], sums)
    ratio_ref[...] = total / pltpu.roll(total, VREG, 1)
    for i in range(ENDS[3], OTHERS):
        copies[i].wait_recv()
    for cp in copies:
        cp.wait_send()
    pltpu.make_async_copy(uin, uin, usend).wait()
    pltpu.make_async_copy(min_, min_, msend).wait()
    out.wait()


def exchange(send_rows, pair_target, pair_slot, src_area, tgt_area, src_field, weights):
    smem = pl.BlockSpec(memory_space=pltpu.SMEM)
    vmem = pl.BlockSpec(memory_space=pltpu.VMEM)
    hbm = pl.BlockSpec(memory_space=pl.ANY)
    dma = pltpu.SemaphoreType.DMA
    return pl.pallas_call(
        exchange_kernel,
        out_shape=[jax.ShapeDtypeStruct((PEERS, CAP, VREG, BLK), jnp.bfloat16),
                   jax.ShapeDtypeStruct((TB, VREG, BLK), jnp.float32),
                   jax.ShapeDtypeStruct((8, PAIRS), jnp.int32),
                   jax.ShapeDtypeStruct((1, BLK), jnp.float32)],
        in_specs=[smem, smem, vmem, vmem, vmem, vmem, hbm, hbm],
        out_specs=[hbm, hbm, vmem, vmem],
        scratch_shapes=[
            pltpu.VMEM((SB, VREG, BLK), jnp.bfloat16),
            pltpu.VMEM((PEERS, CAP, VREG, BLK), jnp.bfloat16),
            pltpu.VMEM((PAIRS, BLK, BLK), jnp.bfloat16),
            pltpu.VMEM((PEERS * CAP, VREG, BLK), jnp.bfloat16),
            pltpu.VMEM((PEERS * CAP, VREG, BLK), jnp.bfloat16),
            pltpu.VMEM((max(ROOM), VREG, BLK), jnp.float32),
            pltpu.VMEM((TB, VREG, BLK), jnp.float32),
            pltpu.VMEM((TB, 16, BLK), jnp.bfloat16),
            pltpu.VMEM((PAIRS, BLK), jnp.float32),
            pltpu.VMEM((PEERS, 1, CAP * BLK), jnp.float32),
            pltpu.VMEM((OTHERS, 1, CAP * BLK), jnp.float32),
            pltpu.VMEM((1, BLK), jnp.float32),
            pltpu.VMEM((OTHERS, 1, BLK), jnp.float32),
            pltpu.SMEM((8, PAIRS), jnp.int32),
            dma, dma, dma((CHUNKS,)), dma((PEERS,)), dma((PEERS,)), dma, dma, dma, dma, dma, dma((PEERS,)), dma,
            pltpu.SemaphoreType.REGULAR((2,)),
        ],
        compiler_params=pltpu.CompilerParams(
            collective_id=0, has_side_effects=True, vmem_limit_bytes=60 * 2**20),
        name="exchange",
    )(send_rows, pair_target, pair_slot, pair_target, src_area, tgt_area, src_field, weights)


HELD = 32


def finish_kernel(table, inb, weights, partial, ratio_ref, out, x, w, acc, scaled, xsem, wsem, asem, osem):
    load = pltpu.make_async_copy(partial, acc, asem)
    load.start()
    ranges = [(jnp.where(g == 0, 0, table[1, max(g * TB - 1, 0)]) + (ROOM[g] if g < GROUPS - 1 else 0),
               table[1, g * TB + TB - 1]) for g in range(GROUPS)]
    step = 8

    def copies(j, u):
        entry = table[0, j]
        slot = lax.shift_right_logical(entry, 6) & 255
        return (pltpu.make_async_copy(inb.at[slot], x.at[u], xsem),
                pltpu.make_async_copy(weights.at[lax.shift_right_logical(entry, 14)], w.at[u], wsem))

    def bring(lo, count):
        def one(u, _):
            for cp in copies(lo + u, u):
                cp.start()
            return 0

        lax.fori_loop(0, count, one, 0)

    def use(lo, count):
        def one(u, _):
            for cp in copies(lo + u, u):
                cp.wait()
            return 0

        lax.fori_loop(0, count, one, 0)

        def some(n, _):
            products = [jnp.dot(x[n * step + u], w[n * step + u], preferred_element_type=jnp.float32)
                        for u in range(step)]
            for u in range(step):
                i = n * step + u
                t = table[0, jnp.minimum(lo + i, PAIRS - 1)] & 63
                acc[t] = acc[t] + jnp.where(i < count, products[u], 0.0)
            return 0

        lax.fori_loop(0, lax.div(count + step - 1, step), some, 0)

    lo, hi = ranges[-1]
    count = jnp.minimum(hi - lo, HELD)
    bring(lo, count)
    ratio = jnp.broadcast_to(ratio_ref[...], (BLK, BLK)).T[:VREG]
    load.wait()
    use(lo, count)
    ranges[-1] = (lo + count, hi)
    for lo, hi in ranges:
        def more(n, _, lo=lo, hi=hi):
            first = lo + n * HELD
            count = jnp.minimum(hi - first, HELD)
            bring(first, count)
            use(first, count)
            return 0

        lax.fori_loop(0, lax.div(jnp.maximum(hi - lo, 0) + HELD - 1, HELD), more, 0)

    parts = 4
    per = TB // parts
    done = []
    for i in range(parts):
        for t in range(i * per, (i + 1) * per):
            scaled[:, t * BLK:(t + 1) * BLK] = acc[t] * ratio
        span = pl.ds(i * per * BLK, per * BLK)
        done.append(pltpu.make_async_copy(scaled.at[:, span], out.at[:, span], osem.at[i]))
        done[-1].start()
    for cp in done:
        cp.wait()


def finish(table, inb, weights, partial, ratio):
    smem = pl.BlockSpec(memory_space=pltpu.SMEM)
    vmem = pl.BlockSpec(memory_space=pltpu.VMEM)
    hbm = pl.BlockSpec(memory_space=pl.ANY)
    dma = pltpu.SemaphoreType.DMA
    return pl.pallas_call(
        finish_kernel,
        out_shape=jax.ShapeDtypeStruct((VREG, TB * BLK), jnp.float32),
        in_specs=[smem, hbm, hbm, hbm, vmem],
        out_specs=hbm,
        scratch_shapes=[
            pltpu.VMEM((HELD, VREG, BLK), jnp.bfloat16),
            pltpu.VMEM((HELD, BLK, BLK), jnp.bfloat16),
            pltpu.VMEM((TB, VREG, BLK), jnp.float32),
            pltpu.VMEM((VREG, TB * BLK), jnp.float32),
            dma, dma, dma, dma((4,)),
        ],
        compiler_params=pltpu.CompilerParams(vmem_limit_bytes=60 * 2**20),
        name="finish",
    )(table, inb, weights, partial, ratio)


def shards(src_field, src_area, tgt_area, weights, send_index, pair_slot, pair_target):
    inb, partial, table, ratio = exchange(
        send_index[0].T, pair_target, pair_slot, src_area.reshape(SB, BLK), tgt_area.reshape(TB, BLK), src_field, weights)
    return finish(table, inb.reshape(PEERS * CAP, VREG, BLK), weights, partial, ratio)


def solution(mesh):
    placed = (P(None, AXES), P(AXES), P(AXES), P(AXES, None, None), P(AXES, None, None), P(AXES), P(AXES))
    return jax.shard_map(shards, mesh=mesh, in_specs=placed, out_specs=P(None, AXES), check_vma=False)
```
